32 devices in a mesh: lat: 8 (over z, x), lon: 4 (over y, core).
Axes of the slice: x: 2, y: 2, z: 4, core: 2. Of those that a mesh axis runs over, the one named last changes fastest.
Arguments:
- increment: bfloat16 [16, 8, 144, 128], P('lat', 'lon'), may hold values from -6 to 6
- cotangent: bfloat16 [8, 4, 40, 144, 128], P('lat', 'lon'), may hold values from -6 to 6
- weights: bfloat16 [8, 4, 40, 16, 128, 128], P('lat', 'lon'), may hold values from -0.1875 to 0.1875
- source_ids: int32 [8, 4, 40, 16], P('lat', 'lon'), may hold values from 0 to 127, as said below
- counts: int32 [8, 4, 40], P('lat', 'lon'), may hold values from 0 to 16, as said below
Outputs:
- ocean: bfloat16 [8, 4, 40, 144, 128], P('lat', 'lon')
- atmos_adjoint: bfloat16 [16, 8, 144, 128], P('lat', 'lon')
The draws below stay inside these ranges and needn't reach their ends.
Inputs may be any that keep to these rules, and one draw needn't show every extreme that they name: source_ids[i, j, t, k] = a * 8 + b with block row a between i * 2 - 1 and (i + 1) * 2, and block column b equal, modulo 8, to one of j * 2 - 1 to (j + 1) * 2. `counts`: every device's tile (i, j) has some target block with exactly 16 live slots.
All inputs are finite; a program needn't handle non-finite values.
Results may differ from the reference program's by a relative error of at most 0.001.
Values may be sent and summed in bfloat16 or wider, within the bound.
A program may use at most 192 MiB of HBM per device.

```python
import jax
import jax.numpy as jnp
from jax import lax

BS = 128
BT = 128
SBD = 2
TB = 40
KPT = 16
ROWS = 144
NLB = 16
NOB = 8
N_LAT = 8
N_LON = 4


def draw_source_ids(key, part):
    key_rows, key_cols = jax.random.split(jax.random.fold_in(key, 11))
    shape = (N_LAT, N_LON, TB, KPT)
    lat_grid = jnp.arange(N_LAT, dtype=jnp.int32)[:, None, None, None]
    lon_grid = jnp.arange(N_LON, dtype=jnp.int32)[None, :, None, None]
    lowest = jnp.where(lat_grid == 0, 1, 0)
    highest = jnp.where(lat_grid == N_LAT - 1, SBD, SBD + 1)
    raw_rows = jax.random.randint(key_rows, shape, 0, 1 << 20)
    ext_row = lowest + raw_rows % (highest - lowest + 1)
    ext_col = jax.random.randint(key_cols, shape, 0, SBD + 2)
    cycle_blocks = SBD * N_LON
    block_row = lat_grid * SBD + ext_row - 1
    block_col = (lon_grid * SBD + ext_col - 1 + cycle_blocks) % cycle_blocks
    return (block_row * cycle_blocks + block_col).astype(jnp.int32)


def draw_counts(key, part):
    key_rows, key_cols = jax.random.split(jax.random.fold_in(key, 23))
    drawn = jax.random.randint(key_rows, (N_LAT, N_LON, TB), 0, KPT + 1)
    full_slot = jax.random.randint(key_cols, (N_LAT, N_LON, 1), 0, TB)
    target_index = jnp.arange(TB, dtype=jnp.int32)[None, None, :]
    return jnp.where(target_index == full_slot, KPT, drawn).astype(jnp.int32)


def block_levels(key, extent, cuts, low, largest):
    factor_of = 1.0
    for dim, blocks in cuts:
        steps = jax.random.uniform(jax.random.fold_in(jax.random.fold_in(key, 6), dim), (blocks,), jnp.float32, low / len(cuts), largest / len(cuts))
        factor_of = factor_of * jnp.repeat(jnp.exp(steps), extent[dim] // blocks).reshape((-1,) + (1,) * (len(extent) - 1 - dim))
    return factor_of


def scatter_about(key, extent, width, limit, cuts=(), kind=jnp.bfloat16):
    gain = block_levels(key, extent, cuts, -0.22, 0.18) if cuts else 1.0
    entries = jax.random.normal(key, extent, jnp.float32) * width * gain
    return jnp.minimum(jnp.maximum(entries, -limit), limit).astype(kind)


def setup_inputs(seed: int = 0) -> dict:
    streams_of = jax.random.split(jax.random.key(seed), 6)
    return {
        "increment": scatter_about(streams_of[0], (NLB, NOB, ROWS, BS), 1.0, 6.0, ((0, 8), (1, 4))),
        "cotangent": scatter_about(streams_of[1], (N_LAT, N_LON, TB, ROWS, BT), 1.0, 6.0, ((0, 8), (1, 4))),
        "weights": scatter_about(streams_of[2], (N_LAT, N_LON, TB, KPT, BS, BT), (BS * KPT // 2) ** -0.5, 0.1875, ((0, 8), (1, 4))),
        "source_ids": draw_source_ids(jax.random.fold_in(streams_of[5], 71), 0),
        "counts": draw_counts(jax.random.fold_in(streams_of[5], 71), 0),
    }


def reference(increment, cotangent, weights, source_ids, counts):
    total_blocks = NLB * NOB
    device_count = N_LAT * N_LON
    flattened = increment.reshape(total_blocks, ROWS, BS)
    weight_all = weights.reshape(device_count, TB, KPT, BS, BT)
    source_all = source_ids.reshape(device_count, TB, KPT).astype(jnp.int32)
    count_all = counts.reshape(device_count, TB).astype(jnp.int32)
    cotan_all = cotangent.reshape(device_count, TB, ROWS, BT)

    def device_step(running, pieces):
        weight_dev, source_dev, count_dev, cotan_dev = pieces
        ocean_sum = jnp.zeros((TB, ROWS, BT), jnp.float32)
        cotan_wide = cotan_dev.astype(jnp.float32)
        for slot in range(KPT):
            active = slot < count_dev
            weight_slot = weight_dev[:, slot].astype(jnp.float32)
            picked = flattened[source_dev[:, slot]].astype(jnp.float32) * active.astype(jnp.float32)[:, None, None]
            ocean_sum = ocean_sum + jnp.einsum("tws,tsb->twb", picked, weight_slot)
            contribution = jnp.einsum("twb,tsb->tws", cotan_wide, weight_slot)
            segment = jnp.where(active, source_dev[:, slot], total_blocks).astype(jnp.int32)
            running = running.at[segment].add(contribution)
        return running, ocean_sum.astype(jnp.bfloat16)

    running = jnp.zeros((total_blocks + 1, ROWS, BS), jnp.float32)
    running, ocean = lax.scan(device_step, running, (weight_all, source_all, count_all, cotan_all))
    ocean = ocean.reshape(N_LAT, N_LON, TB, ROWS, BT)
    adjoint_out = running[:total_blocks].reshape(NLB, NOB, ROWS, BS).astype(jnp.bfloat16)
    return ocean, adjoint_out
```

```python
import functools

import jax
import jax.numpy as jnp
from jax import lax
from jax.experimental import pallas as pl
from jax.experimental.pallas import tpu as pltpu
from jax.sharding import PartitionSpec as P

GROUP = 4


def shifted(value, by_lat, by_lon):
    lats, lons = lax.axis_size("lat"), lax.axis_size("lon")
    route = []
    for i in range(lats):
        for j in range(lons):
            if 0 <= i + by_lat < lats:
                route.append((i * lons + j, (i + by_lat) * lons + (j + by_lon) % lons))
    return lax.ppermute(value, ("lat", "lon"), route)


def slot_place(ids_ref, t, k, live, side, lon_count):
    cycle = side * lon_count
    source = ids_ref[0, 0, t, k]
    row = lax.div(source, cycle)
    col = source - row * cycle
    ext_row = row - lax.axis_index("lat") * side + 1
    ext_col = col - lax.axis_index("lon") * side + 1
    ext_col = jnp.where(ext_col < 0, ext_col + cycle, ext_col)
    ext_col = jnp.where(ext_col >= cycle, ext_col - cycle, ext_col)
    width = side + 2
    return jnp.where(k < live, ext_row * width + ext_col, width * width)


def groups_of(live):
    return lax.div(live + (GROUP - 1), GROUP)


def weight_copy(w_ref, w_vmem, sems, t, g):
    return pltpu.make_async_copy(
        w_ref.at[0, 0, t, pl.ds(g * GROUP, GROUP)],
        w_vmem.at[t, pl.ds(g * GROUP, GROUP)],
        sems.at[t, g],
    )


def start_weights(counts_ref, w_ref, w_vmem, sems):
    targets = w_vmem.shape[0]

    @pl.loop(0, targets)
    def _(t):
        @pl.loop(0, groups_of(counts_ref[0, 0, t]))
        def _(g):
            weight_copy(w_ref, w_vmem, sems, t, g).start()


def over_targets(counts_ref, w_ref, w_vmem, sems, work):
    targets, slots = w_vmem.shape[:2]

    @pl.loop(0, targets)
    def _(t):
        live = counts_ref[0, 0, t]
        groups = groups_of(live)

        @pl.loop(0, groups)
        def _(g):
            weight_copy(w_ref, w_vmem, sems, t, g).wait()

        for n in range(slots // GROUP + 1):
            @pl.when(groups == n)
            def _(n=n):
                work(t, live, n)


def pieces_of(side):
    inner = range(1, side + 1)
    last = side + 1
    return (
        (inner, inner),
        ((0,), inner), ((last,), inner), (inner, (0,)), (inner, (last,)),
        ((0,), (0,)), ((0,), (last,)), ((last,), (0,)), ((last,), (last,)),
    )


def adjoint_kernel(side, lon_count, ids_ref, counts_ref, cot_ref, w_ref, *rest):
    out_refs, (acc, w_vmem, sems) = rest[:-3], rest[-3:]
    start_weights(counts_ref, w_ref, w_vmem, sems)
    acc[...] = jnp.zeros_like(acc)

    def work(t, live, n):
        cot = cot_ref[0, 0, t]
        cells = cot.shape[-1]
        for k in range(0, n * GROUP, 2):
            pair = jnp.concatenate([w_vmem[t, k], w_vmem[t, k + 1]], axis=0)
            both = lax.dot_general(
                cot, pair, (((1,), (1,)), ((), ())), preferred_element_type=jnp.float32
            )
            half = both.shape[-1] // 2
            for m in range(2):
                place = slot_place(ids_ref, t, k + m, live, side, lon_count)
                acc[place] += both[:, m * half:(m + 1) * half]

    over_targets(counts_ref, w_ref, w_vmem, sems, work)
    width = side + 2
    for out, (rows, cols) in zip(out_refs, pieces_of(side)):
        for a, row in enumerate(rows):
            for b, col in enumerate(cols):
                out[a, b] = acc[row * width + col]


def tangent_kernel(side, lon_count, ids_ref, counts_ref, w_ref, *rest):
    in_refs, (out_ref, ext, w_vmem, sems) = rest[:-4], rest[-4:]
    start_weights(counts_ref, w_ref, w_vmem, sems)
    width = side + 2
    for piece, (rows, cols) in zip(in_refs, pieces_of(side)):
        for a, row in enumerate(rows):
            for b, col in enumerate(cols):
                ext[row * width + col] = piece[a, b]
    ext[width * width] = jnp.zeros(ext.shape[1:], ext.dtype)

    def work(t, live, n):
        if n == 0:
            out_ref[0, 0, t] = jnp.zeros(out_ref.shape[3:], out_ref.dtype)
            return
        picked = jnp.concatenate(
            [ext[slot_place(ids_ref, t, k, live, side, lon_count)] for k in range(n * GROUP)],
            axis=1,
        )
        blocks = w_vmem[t, 0:n * GROUP]
        blocks = blocks.reshape(blocks.shape[0] * blocks.shape[1], blocks.shape[2])
        total = jnp.dot(picked, blocks, preferred_element_type=jnp.float32)
        out_ref[0, 0, t] = total.astype(out_ref.dtype)

    over_targets(counts_ref, w_ref, w_vmem, sems, work)


def body(increment, cotangent, weights, source_ids, counts):
    side, _, levels, cells = increment.shape
    targets, slots = weights.shape[2:4]
    lon_count = lax.axis_size("lon")
    total = (side + 2) * (side + 2)
    smem = pl.BlockSpec(memory_space=pltpu.SMEM)
    vmem = pl.BlockSpec(memory_space=pltpu.VMEM)
    hbm = pl.BlockSpec(memory_space=pl.ANY)
    shapes = [(len(r), len(c), levels, cells) for r, c in pieces_of(side)]
    scratch = [
        pltpu.VMEM(weights.shape[2:], weights.dtype),
        pltpu.SemaphoreType.DMA((targets, slots // GROUP)),
    ]
    flops = targets * slots * levels * cells * cells
    cost = pl.CostEstimate(flops=flops, bytes_accessed=weights.size, transcendentals=0)
    params = pltpu.CompilerParams(vmem_limit_bytes=48 * 1024 * 1024)

    first, final = slice(0, 1), slice(-1, None)
    full = slice(None)
    halo = [
        shifted(increment[a, b], i, j)
        for a, b, i, j in (
            (final, full, 1, 0), (first, full, -1, 0), (full, final, 0, 1), (full, first, 0, -1),
            (final, final, 1, 1), (final, first, 1, -1), (first, final, -1, 1), (first, first, -1, -1),
        )
    ]

    sums = pl.pallas_call(
        functools.partial(adjoint_kernel, side, lon_count),
        out_shape=[jax.ShapeDtypeStruct(s, jnp.float32) for s in shapes],
        in_specs=[smem, smem, vmem, hbm],
        out_specs=[vmem] * len(shapes),
        scratch_shapes=[pltpu.VMEM((total + 1, levels, cells), jnp.float32)] + scratch,
        compiler_params=params,
        cost_estimate=cost,
        name="adjoint",
    )(source_ids, counts, cotangent, weights)
    middle, north, south, west, east, nw, ne, sw, se = sums
    from_south = shifted(north, -1, 0)
    from_north = shifted(south, 1, 0)
    from_east = shifted(west, 0, -1)
    from_west = shifted(east, 0, 1)
    from_se = shifted(nw, -1, -1)
    from_sw = shifted(ne, -1, 1)
    from_ne = shifted(sw, 1, -1)
    from_nw = shifted(se, 1, 1)

    ocean = pl.pallas_call(
        functools.partial(tangent_kernel, side, lon_count),
        out_shape=jax.ShapeDtypeStruct(cotangent.shape, jnp.bfloat16),
        in_specs=[smem, smem, hbm] + [vmem] * len(shapes),
        out_specs=vmem,
        scratch_shapes=[pltpu.VMEM((total + 1, levels, cells), increment.dtype)] + scratch,
        compiler_params=params,
        cost_estimate=cost,
        name="tangent",
    )(source_ids, counts, weights, increment, *halo)

    def at(value, top, left):
        down, across = side - value.shape[0], side - value.shape[1]
        pads = ((0, down) if top else (down, 0), (0, across) if left else (across, 0))
        return jnp.pad(value, pads + ((0, 0), (0, 0)))

    folded = middle + at(from_north, True, True) + at(from_south, False, True)
    folded = folded + at(from_west, True, True) + at(from_east, True, False)
    folded = folded + at(from_nw, True, True) + at(from_ne, True, False)
    folded = folded + at(from_sw, False, True) + at(from_se, False, False)
    return ocean, folded.astype(jnp.bfloat16)


def solution(mesh):
    placed = (
        P("lat", "lon", None, None),
        P("lat", "lon", None, None, None),
        P("lat", "lon", None, None, None, None),
        P("lat", "lon", None, None),
        P("lat", "lon", None),
    )
    return jax.shard_map(
        body,
        mesh=mesh,
        in_specs=placed,
        out_specs=(P("lat", "lon", None, None, None), P("lat", "lon", None, None)),
        check_vma=False,
    )
```

```python
import functools

import jax
import jax.numpy as jnp
from jax import lax
from jax.experimental import pallas as pl
from jax.experimental.pallas import tpu as pltpu
from jax.sharding import PartitionSpec as P

GROUP = 4
WAYS = ((1, 1), (1, -1), (-1, 1), (-1, -1), (1, 0), (-1, 0), (0, 1), (0, -1))


def sent_span(by, side):
    return pl.ds(side - 1 if by > 0 else 0, 1 if by else side)


def held_span(by, side):
    return pl.ds(0 if by > 0 else (side + 1 if by < 0 else 1), 1 if by else side)


def greet(sizes):
    lats, lons = sizes
    lat, lon = lax.axis_index("lat"), lax.axis_index("lon")
    barrier = pltpu.get_barrier_semaphore()
    for i, j in WAYS:
        @pl.when((lat + i >= 0) & (lat + i < lats))
        def _(i=i, j=j):
            pl.semaphore_signal(
                barrier,
                inc=1,
                device_id=(lat + i, lax.rem(lon + j + lons, lons)),
                device_id_type=pl.DeviceIdType.MESH,
            )
    north = (lat > 0).astype(jnp.int32)
    south = (lat < lats - 1).astype(jnp.int32)
    pl.semaphore_wait(barrier, 2 + 3 * north + 3 * south)


def send_all(sizes, source, landing, send_sems, recv_sems):
    lats, lons = sizes
    lat, lon = lax.axis_index("lat"), lax.axis_index("lon")
    for way, (i, j) in enumerate(WAYS):
        @pl.when((lat + i >= 0) & (lat + i < lats))
        def _(way=way, i=i, j=j):
            pltpu.make_async_remote_copy(
                src_ref=source(i, j),
                dst_ref=landing(way, i, j),
                send_sem=send_sems.at[way],
                recv_sem=recv_sems.at[way],
                device_id=(lat + i, lax.rem(lon + j + lons, lons)),
                device_id_type=pl.DeviceIdType.MESH,
            ).start()


def await_way(sizes, source, landing, send_sems, recv_sems, way, then=None, otherwise=None):
    lats, lons = sizes
    lat, lon = lax.axis_index("lat"), lax.axis_index("lon")
    i, j = WAYS[way]
    copy = pltpu.make_async_remote_copy(
        src_ref=source(i, j),
        dst_ref=landing(way, i, j),
        send_sem=send_sems.at[way],
        recv_sem=recv_sems.at[way],
        device_id=(lat, lax.rem(lon + 1, lons)),
        device_id_type=pl.DeviceIdType.MESH,
    )

    @pl.when((lat - i >= 0) & (lat - i < lats))
    def _():
        copy.wait_recv()
        if then is not None:
            then()

    if otherwise is not None:
        @pl.when((lat - i < 0) | (lat - i >= lats))
        def _():
            otherwise()

    @pl.when((lat + i >= 0) & (lat + i < lats))
    def _():
        copy.wait_send()


def halo_kernel(sizes, own_ref, ext_ref, send_sems, recv_sems):
    side = own_ref.shape[0]

    def source(i, j):
        return own_ref.at[sent_span(i, side), sent_span(j, side)]

    def landing(way, i, j):
        return ext_ref.at[held_span(i, side), held_span(j, side)]

    greet(sizes)
    send_all(sizes, source, landing, send_sems, recv_sems)
    ext_ref[1:side + 1, 1:side + 1] = own_ref[...]
    for way, (i, j) in enumerate(WAYS):
        def clear(i=i, j=j):
            rows, cols = held_span(i, side), held_span(j, side)
            ext_ref[rows, cols] = jnp.zeros((rows.size, cols.size) + ext_ref.shape[2:], ext_ref.dtype)

        await_way(
            sizes, source, landing, send_sems, recv_sems, way, otherwise=clear if i else None
        )


def fold_kernel(sizes, part_ref, out_ref, *rest):
    acc, send_sems, recv_sems = rest[-3:]
    held = rest[:-3]
    side = out_ref.shape[0]

    def away(by):
        return pl.ds(side + 1 if by > 0 else (0 if by < 0 else 1), 1 if by else side)

    def source(i, j):
        return part_ref.at[away(i), away(j)]

    def landing(way, i, j):
        return held[way]

    greet(sizes)
    send_all(sizes, source, landing, send_sems, recv_sems)
    acc[...] = part_ref[1:side + 1, 1:side + 1]
    for way in reversed(range(len(WAYS))):
        i, j = WAYS[way]

        def add(way=way, i=i, j=j):
            rows = pl.ds(0 if i >= 0 else side - 1, 1 if i else side)
            cols = pl.ds(0 if j >= 0 else side - 1, 1 if j else side)
            acc[rows, cols] += held[way][...]

        await_way(sizes, source, landing, send_sems, recv_sems, way, then=add)
    out_ref[...] = acc[...].astype(out_ref.dtype)


def slot_place(ids_ref, t, k, live, side, lon_count):
    cycle = side * lon_count
    source = ids_ref[0, 0, t, k]
    row = lax.div(source, cycle)
    col = source - row * cycle
    ext_row = row - lax.axis_index("lat") * side + 1
    ext_col = col - lax.axis_index("lon") * side + 1
    ext_col = jnp.where(ext_col < 0, ext_col + cycle, ext_col)
    ext_col = jnp.where(ext_col >= cycle, ext_col - cycle, ext_col)
    width = side + 2
    return jnp.where(k < live, ext_row * width + ext_col, width * width)


def groups_of(live):
    return lax.div(live + (GROUP - 1), GROUP)


def weight_copy(w_ref, w_vmem, sems, t, g):
    return pltpu.make_async_copy(
        w_ref.at[0, 0, t, pl.ds(g * GROUP, GROUP)],
        w_vmem.at[t, pl.ds(g * GROUP, GROUP)],
        sems.at[t, g],
    )


def compute_kernel(
    side, lon_count, ids_ref, counts_ref, ext_ref, cot_ref, w_ref,
    ocean_ref, part_ref, ext, acc, w_vmem, sems,
):
    targets, slots = w_vmem.shape[:2]
    width = side + 2

    @pl.loop(0, targets)
    def _(t):
        groups = groups_of(counts_ref[0, 0, t])
        for g in range(slots // GROUP):
            @pl.when(g < groups)
            def _(g=g):
                weight_copy(w_ref, w_vmem, sems, t, g).start()

    ext[0:width * width] = ext_ref[...].reshape((width * width,) + ext.shape[1:])
    ext[width * width] = jnp.zeros(ext.shape[1:], ext.dtype)
    acc[...] = jnp.zeros_like(acc)

    def work(t, live, n):
        if n == 0:
            ocean_ref[0, 0, t] = jnp.zeros(ocean_ref.shape[3:], ocean_ref.dtype)
            return
        for g in range(n):
            weight_copy(w_ref, w_vmem, sems, t, g).wait()
        places = [slot_place(ids_ref, t, k, live, side, lon_count) for k in range(n * GROUP)]
        cot = cot_ref[0, 0, t]
        picked = jnp.concatenate([ext[p] for p in places], axis=1)
        blocks = w_vmem[t, 0:n * GROUP]
        blocks = blocks.reshape(blocks.shape[0] * blocks.shape[1], blocks.shape[2])
        total = jnp.dot(picked, blocks, preferred_element_type=jnp.float32)
        ocean_ref[0, 0, t] = total.astype(ocean_ref.dtype)
        cells = w_vmem.shape[2]
        for k in range(0, n * GROUP, 2):
            both = lax.dot_general(
                cot,
                blocks[k * cells:(k + 2) * cells],
                (((1,), (1,)), ((), ())),
                preferred_element_type=jnp.float32,
            )
            for m in range(2):
                acc[places[k + m]] += both[:, m * cells:(m + 1) * cells]

    @pl.loop(0, targets)
    def _(t):
        live = counts_ref[0, 0, t]
        groups = groups_of(live)
        for n in range(slots // GROUP + 1):
            @pl.when(groups == n)
            def _(n=n):
                work(t, live, n)

    part_ref[...] = acc[0:width * width].reshape(part_ref.shape)


def compute(side, lon_count, source_ids, counts, ext, cotangent, weights):
    smem = pl.BlockSpec(memory_space=pltpu.SMEM)
    vmem = pl.BlockSpec(memory_space=pltpu.VMEM)
    hbm = pl.BlockSpec(memory_space=pl.ANY)
    targets, slots = weights.shape[2:4]
    width, tail = side + 2, ext.shape[2:]
    flops = 4 * targets * slots * tail[0] * tail[1] * tail[1]
    return pl.pallas_call(
        functools.partial(compute_kernel, side, lon_count),
        out_shape=[
            jax.ShapeDtypeStruct(cotangent.shape, jnp.bfloat16),
            jax.ShapeDtypeStruct(ext.shape, jnp.float32),
        ],
        in_specs=[smem, smem, vmem, vmem, hbm],
        out_specs=[vmem, vmem],
        scratch_shapes=[
            pltpu.VMEM((width * width + 1,) + tail, ext.dtype),
            pltpu.VMEM((width * width + 1,) + tail, jnp.float32),
            pltpu.VMEM(weights.shape[2:], weights.dtype),
            pltpu.SemaphoreType.DMA((targets, slots // GROUP)),
        ],
        compiler_params=pltpu.CompilerParams(vmem_limit_bytes=48 * 1024 * 1024),
        cost_estimate=pl.CostEstimate(
            flops=flops, bytes_accessed=weights.size * 2, transcendentals=0
        ),
        name="products",
    )(source_ids, counts, ext, cotangent, weights)


def body(increment, cotangent, weights, source_ids, counts):
    side, _, levels, cells = increment.shape
    sizes = lax.axis_size("lat"), lax.axis_size("lon")
    vmem = pl.BlockSpec(memory_space=pltpu.VMEM)
    ways = len(WAYS)
    wide = (side + 2, side + 2, levels, cells)
    sems = [pltpu.SemaphoreType.DMA((ways,)), pltpu.SemaphoreType.DMA((ways,))]
    ext = pl.pallas_call(
        functools.partial(halo_kernel, sizes),
        out_shape=jax.ShapeDtypeStruct(wide, increment.dtype),
        in_specs=[vmem],
        out_specs=vmem,
        scratch_shapes=sems,
        compiler_params=pltpu.CompilerParams(collective_id=0, has_side_effects=True),
        name="halo",
    )(increment)
    ocean, part = compute(side, sizes[1], source_ids, counts, ext, cotangent, weights)
    landings = [
        pltpu.VMEM((1 if i else side, 1 if j else side, levels, cells), jnp.float32)
        for i, j in WAYS
    ]
    folded = pl.pallas_call(
        functools.partial(fold_kernel, sizes),
        out_shape=jax.ShapeDtypeStruct(increment.shape, jnp.bfloat16),
        in_specs=[vmem],
        out_specs=vmem,
        scratch_shapes=landings + [pltpu.VMEM(increment.shape, jnp.float32)] + sems,
        compiler_params=pltpu.CompilerParams(collective_id=1, has_side_effects=True),
        name="fold",
    )(part)
    return ocean, folded


def solution(mesh):
    placed = (
        P("lat", "lon", None, None),
        P("lat", "lon", None, None, None),
        P("lat", "lon", None, None, None, None),
        P("lat", "lon", None, None),
        P("lat", "lon", None),
    )
    return jax.shard_map(
        body,
        mesh=mesh,
        in_specs=placed,
        out_specs=(P("lat", "lon", None, None, None), P("lat", "lon", None, None)),
        check_vma=False,
    )
```

```python
import functools

import jax
import jax.numpy as jnp
from jax import lax
from jax.experimental import pallas as pl
from jax.experimental.pallas import tpu as pltpu
from jax.sharding import PartitionSpec as P

GROUP = 4
WAYS = ((1, 1), (1, -1), (-1, 1), (-1, -1), (1, 0), (-1, 0), (0, 1), (0, -1))


def sent_span(by, side):
    return pl.ds(side - 1 if by > 0 else 0, 1 if by else side)


def held_span(by, side):
    return pl.ds(0 if by > 0 else (side + 1 if by < 0 else 1), 1 if by else side)


def greet(sizes):
    lats, lons = sizes
    lat, lon = lax.axis_index("lat"), lax.axis_index("lon")
    barrier = pltpu.get_barrier_semaphore()
    for i, j in WAYS:
        @pl.when((lat + i >= 0) & (lat + i < lats))
        def _(i=i, j=j):
            pl.semaphore_signal(
                barrier,
                inc=1,
                device_id=(lat + i, lax.rem(lon + j + lons, lons)),
                device_id_type=pl.DeviceIdType.MESH,
            )
    north = (lat > 0).astype(jnp.int32)
    south = (lat < lats - 1).astype(jnp.int32)
    pl.semaphore_wait(barrier, 2 + 3 * north + 3 * south)


def send_all(sizes, source, landing, send_sems, recv_sems):
    lats, lons = sizes
    lat, lon = lax.axis_index("lat"), lax.axis_index("lon")
    for way, (i, j) in enumerate(WAYS):
        @pl.when((lat + i >= 0) & (lat + i < lats))
        def _(way=way, i=i, j=j):
            pltpu.make_async_remote_copy(
                src_ref=source(i, j),
                dst_ref=landing(way, i, j),
                send_sem=send_sems.at[way],
                recv_sem=recv_sems.at[way],
                device_id=(lat + i, lax.rem(lon + j + lons, lons)),
                device_id_type=pl.DeviceIdType.MESH,
            ).start()


def await_way(sizes, source, landing, send_sems, recv_sems, way, then=None, otherwise=None):
    lats, lons = sizes
    lat, lon = lax.axis_index("lat"), lax.axis_index("lon")
    i, j = WAYS[way]
    copy = pltpu.make_async_remote_copy(
        src_ref=source(i, j),
        dst_ref=landing(way, i, j),
        send_sem=send_sems.at[way],
        recv_sem=recv_sems.at[way],
        device_id=(lat, lax.rem(lon + 1, lons)),
        device_id_type=pl.DeviceIdType.MESH,
    )

    @pl.when((lat - i >= 0) & (lat - i < lats))
    def _():
        copy.wait_recv()
        if then is not None:
            then()

    if otherwise is not None:
        @pl.when((lat - i < 0) | (lat - i >= lats))
        def _():
            otherwise()

    @pl.when((lat + i >= 0) & (lat + i < lats))
    def _():
        copy.wait_send()


def slot_place(ids_ref, t, k, live, side, lon_count):
    cycle = side * lon_count
    source = ids_ref[0, 0, t, k]
    row = lax.div(source, cycle)
    col = source - row * cycle
    ext_row = row - lax.axis_index("lat") * side + 1
    ext_col = col - lax.axis_index("lon") * side + 1
    ext_col = jnp.where(ext_col < 0, ext_col + cycle, ext_col)
    ext_col = jnp.where(ext_col >= cycle, ext_col - cycle, ext_col)
    width = side + 2
    return jnp.where(k < live, ext_row * width + ext_col, width * width)


def groups_of(live):
    return lax.div(live + (GROUP - 1), GROUP)


def weight_copy(w_ref, w_vmem, sems, t, g):
    return pltpu.make_async_copy(
        w_ref.at[0, 0, t, pl.ds(g * GROUP, GROUP)],
        w_vmem.at[t, pl.ds(g * GROUP, GROUP)],
        sems.at[t, g],
    )


def adjoint_kernel(
    side, lon_count, ids_ref, counts_ref, cot_ref, w_ref, part_ref, acc, w_vmem, sems
):
    targets, slots = w_vmem.shape[:2]
    width = side + 2

    @pl.loop(0, targets)
    def _(t):
        groups = groups_of(counts_ref[0, 0, t])
        for g in range(slots // GROUP):
            @pl.when(g < groups)
            def _(g=g):
                weight_copy(w_ref, w_vmem, sems, t, g).start()

    acc[...] = jnp.zeros_like(acc)

    def work(t, live, n):
        for g in range(n):
            weight_copy(w_ref, w_vmem, sems, t, g).wait()
        places = [slot_place(ids_ref, t, k, live, side, lon_count) for k in range(n * GROUP)]
        cot = cot_ref[0, 0, t]
        cells = w_vmem.shape[2]
        for k in range(0, n * GROUP, 2):
            pair = w_vmem[t, k:k + 2].reshape(2 * cells, w_vmem.shape[3])
            both = lax.dot_general(
                cot, pair, (((1,), (1,)), ((), ())), preferred_element_type=jnp.float32
            )
            for m in range(2):
                acc[places[k + m]] += both[:, m * cells:(m + 1) * cells]

    @pl.loop(0, targets)
    def _(t):
        live = counts_ref[0, 0, t]
        groups = groups_of(live)
        for n in range(1, slots // GROUP + 1):
            @pl.when(groups == n)
            def _(n=n):
                work(t, live, n)

    part_ref[...] = acc[0:width * width].reshape(part_ref.shape)


def exchange_kernel(
    sizes, ids_ref, counts_ref, own_ref, part_ref, w_ref, ocean_ref, out_ref, *rest
):
    ways = len(WAYS)
    held = rest[:ways]
    acc, halo, ext, w_vmem, w_sems, halo_send, halo_recv, fold_send, fold_recv = rest[ways:]
    side = out_ref.shape[0]
    width = side + 2
    targets, slots = w_vmem.shape[:2]

    def weights_of(t):
        return pltpu.make_async_copy(w_ref.at[0, 0, t], w_vmem.at[t], w_sems.at[t])

    @pl.loop(0, targets)
    def _(t):
        weights_of(t).start()

    def own_edge(i, j):
        return own_ref.at[sent_span(i, side), sent_span(j, side)]

    def halo_slot(way, i, j):
        return halo.at[held_span(i, side), held_span(j, side)]

    def away(by):
        return pl.ds(side + 1 if by > 0 else (0 if by < 0 else 1), 1 if by else side)

    def part_edge(i, j):
        return part_ref.at[away(i), away(j)]

    def fold_slot(way, i, j):
        return held[way]

    greet(sizes)
    send_all(sizes, own_edge, halo_slot, halo_send, halo_recv)
    send_all(sizes, part_edge, fold_slot, fold_send, fold_recv)
    halo[1:side + 1, 1:side + 1] = own_ref[...]
    ext[width * width] = jnp.zeros(ext.shape[1:], ext.dtype)
    acc[...] = part_ref[1:side + 1, 1:side + 1]
    for way, (i, j) in enumerate(WAYS):
        def clear(i=i, j=j):
            rows, cols = held_span(i, side), held_span(j, side)
            halo[rows, cols] = jnp.zeros((rows.size, cols.size) + halo.shape[2:], halo.dtype)

        await_way(
            sizes, own_edge, halo_slot, halo_send, halo_recv, way, otherwise=clear if i else None
        )
    ext[0:width * width] = halo[...].reshape((width * width,) + ext.shape[1:])

    @pl.loop(0, targets)
    def _(t):
        weights_of(t).wait()
        live = counts_ref[0, 0, t]
        picked = jnp.concatenate(
            [ext[slot_place(ids_ref, t, k, live, side, sizes[1])] for k in range(slots)], axis=1
        )
        blocks = w_vmem[t].reshape(slots * w_vmem.shape[2], w_vmem.shape[3])
        total = jnp.dot(picked, blocks, preferred_element_type=jnp.float32)
        ocean_ref[0, 0, t] = total.astype(ocean_ref.dtype)

    for way in reversed(range(ways)):
        i, j = WAYS[way]

        def add(way=way, i=i, j=j):
            rows = pl.ds(0 if i >= 0 else side - 1, 1 if i else side)
            cols = pl.ds(0 if j >= 0 else side - 1, 1 if j else side)
            acc[rows, cols] += held[way][...]

        await_way(sizes, part_edge, fold_slot, fold_send, fold_recv, way, then=add)
    out_ref[...] = acc[...].astype(out_ref.dtype)


def body(increment, cotangent, weights, source_ids, counts):
    side, _, levels, cells = increment.shape
    sizes = lax.axis_size("lat"), lax.axis_size("lon")
    smem = pl.BlockSpec(memory_space=pltpu.SMEM)
    vmem = pl.BlockSpec(memory_space=pltpu.VMEM)
    hbm = pl.BlockSpec(memory_space=pl.ANY)
    targets, slots = weights.shape[2:4]
    ways, width = len(WAYS), side + 2
    wide = (width, width, levels, cells)
    flat = (width * width + 1, levels, cells)
    cost = pl.CostEstimate(
        flops=2 * targets * slots * levels * cells * cells,
        bytes_accessed=weights.size * 2,
        transcendentals=0,
    )
    limit = 48 * 1024 * 1024
    part = pl.pallas_call(
        functools.partial(adjoint_kernel, side, sizes[1]),
        out_shape=jax.ShapeDtypeStruct(wide, jnp.float32),
        in_specs=[smem, smem, vmem, hbm],
        out_specs=vmem,
        scratch_shapes=[
            pltpu.VMEM(flat, jnp.float32),
            pltpu.VMEM(weights.shape[2:], weights.dtype),
            pltpu.SemaphoreType.DMA((targets, slots // GROUP)),
        ],
        compiler_params=pltpu.CompilerParams(vmem_limit_bytes=limit),
        cost_estimate=cost,
        name="adjoint",
    )(source_ids, counts, cotangent, weights)
    landings = [
        pltpu.VMEM((1 if i else side, 1 if j else side, levels, cells), jnp.float32)
        for i, j in WAYS
    ]
    return pl.pallas_call(
        functools.partial(exchange_kernel, sizes),
        out_shape=[
            jax.ShapeDtypeStruct(cotangent.shape, jnp.bfloat16),
            jax.ShapeDtypeStruct(increment.shape, jnp.bfloat16),
        ],
        in_specs=[smem, smem, vmem, vmem, hbm],
        out_specs=[vmem, vmem],
        scratch_shapes=landings + [
            pltpu.VMEM(increment.shape, jnp.float32),
            pltpu.VMEM(wide, increment.dtype),
            pltpu.VMEM(flat, increment.dtype),
            pltpu.VMEM(weights.shape[2:], weights.dtype),
            pltpu.SemaphoreType.DMA((targets,)),
        ] + [pltpu.SemaphoreType.DMA((ways,))] * 4,
        compiler_params=pltpu.CompilerParams(
            collective_id=0, has_side_effects=True, vmem_limit_bytes=limit
        ),
        cost_estimate=cost,
        name="exchange",
    )(source_ids, counts, increment, part, weights)


def solution(mesh):
    placed = (
        P("lat", "lon", None, None),
        P("lat", "lon", None, None, None),
        P("lat", "lon", None, None, None, None),
        P("lat", "lon", None, None),
        P("lat", "lon", None),
    )
    return jax.shard_map(
        body,
        mesh=mesh,
        in_specs=placed,
        out_specs=(P("lat", "lon", None, None, None), P("lat", "lon", None, None)),
        check_vma=False,
    )
```
